32 devices in a mesh: seq: 8 (over z, y), frame: 4 (over x, core).
Axes of the slice: x: 2, y: 2, z: 4, core: 2. Of those that a mesh axis runs over, the one named last changes fastest.
Arguments:
- patches: bfloat16 [3072, 1280], P('frame'), may hold values from -4 to 4
- vit_gain: float32 [1280], replicated, may hold values from 0.5 to 1.5
- vision_qkv: bfloat16 [1280, 3840], P(None, 'seq')
- vision_out: bfloat16 [1280, 1280], P('seq'), may hold values from -0.15625 to 0.15625
- video_ids: int32 [768], replicated, may hold values from 0 to 2, never falling along the last dimension, each value on 1 to 480 neighbouring positions
- merge_gain: float32 [1280], replicated, may hold values from 0.5 to 1.5
- merge_up: bfloat16 [5120, 5120], P(None, 'seq'), may hold values from -0.078125 to 0.078125
- merge_down: bfloat16 [5120, 8192], P('seq')
- vision_pos: int32 [768], replicated, may hold values from 0 to 4095, as said below
- text_embed: bfloat16 [4096, 8192], P(('seq', 'frame')), may hold values from -6 to 6
- llm_gain: float32 [8192], replicated, may hold values from 0.5 to 1.5
- query_weight: bfloat16 [8192, 2048], P(None, 'frame')
- keyvalue_weight: bfloat16 [8192, 1024], P(None, 'frame')
Outputs:
- context: bfloat16 [4096, 2048], P('seq', 'frame')
The draws below stay inside these ranges and needn't reach their ends.
Inputs may be any that keep to these rules, and one draw needn't show every extreme that they name: `vision_pos`: distinct positions. Of the tokens in rows f * 192 to (f + 1) * 192 - 1, for any f, at most 36 lie in one block of 512 positions that starts at a multiple of 512; some block holds exactly 36 of them for every f. `video_ids`: the tokens of one video are consecutive rows.
All inputs are finite; a program needn't handle non-finite values.
Results may differ from the reference program's by a relative error of at most 0.02.
Values may be sent and summed in bfloat16 or wider, within the bound.
A program may use at most 128 MiB of HBM per device.

```python
import math
import jax
import jax.numpy as jnp
import numpy as np
from jax import lax

VIT_HEADS = 16
VIT_HDIM = 80
D_VIT = 1280
MRG_HID = 5120
D = 8192
HDIM = 128
QPK = 4
KV_HEADS = 4
VIS_DEV = 192
SEQ_DEV = 512
VIS = 768
PATCHES = 3072
D_MRG = 5120
SEQ = 4096


def draw_vision_qkv(key, part):
    base = jax.random.normal(jax.random.fold_in(key, 3), (D_VIT, VIT_HEADS, 3, VIT_HDIM), jnp.float32) * D_VIT ** (-0.5)
    lifted = base * jnp.array([1.6, 1.6, 1.0], jnp.float32)[None, None, :, None]
    return lifted.reshape(D_VIT, VIT_HEADS * 3 * VIT_HDIM).astype(jnp.bfloat16)


def draw_merge_down(key, part):
    base = jax.random.normal(jax.random.fold_in(key, 41), (MRG_HID, D), jnp.float32) * MRG_HID ** (-0.5)
    direction = jax.random.normal(jax.random.fold_in(key, 42), (D,), jnp.float32)
    lift = 3.0 / MRG_HID
    return (base + lift * direction[None, :]).astype(jnp.bfloat16)


def language_weights(key):
    query_part = jax.random.normal(jax.random.fold_in(key, 21), (D, KV_HEADS, QPK, HDIM), jnp.float32) * (1.6 * D ** (-0.5))
    pair_part = jax.random.normal(jax.random.fold_in(key, 22), (D, KV_HEADS, 2, HDIM), jnp.float32) * D ** (-0.5)
    pair_part = pair_part * jnp.array([1.6, 1.0], jnp.float32)[None, None, :, None]
    return (query_part, pair_part)


def draw_query_weight(key, part):
    query_part, pair_part = language_weights(key)
    return query_part.reshape(D, KV_HEADS * QPK * HDIM).astype(jnp.bfloat16)


def draw_keyvalue_weight(key, part):
    query_part, pair_part = language_weights(key)
    return pair_part.reshape(D, KV_HEADS * 2 * HDIM).astype(jnp.bfloat16)


def draw_vision_pos(key, part):
    frame_total = VIS // VIS_DEV
    block_total = SEQ // SEQ_DEV
    share = VIS_DEV // (2 * block_total)
    order_key = jax.random.fold_in(key, 31)
    place_key = jax.random.fold_in(key, 32)
    hot_block = jax.random.randint(jax.random.fold_in(key, 33), (), 0, block_total).astype(jnp.int32)
    ranking = jax.vmap(lambda single: jax.random.permutation(single, block_total))(jax.random.split(order_key, frame_total)).astype(jnp.int32)
    block_ids = jnp.arange(block_total, dtype=jnp.int32)[None, :]
    hot_rank = jnp.sum(jnp.where(block_ids == hot_block, ranking, 0), axis=1, keepdims=True)
    ranking = jnp.where(block_ids == hot_block, 0, jnp.where(ranking == 0, hot_rank, ranking))
    counts = jnp.where(ranking < block_total // 2, 3 * share, share).astype(jnp.int32)
    block_ends = jnp.cumsum(counts, axis=1)
    block_starts = block_ends - counts
    token_ids = jnp.arange(VIS_DEV, dtype=jnp.int32)
    chosen = jnp.sum((block_ends[:, None, :] <= token_ids[None, :, None]).astype(jnp.int32), axis=2)
    within_own = token_ids[None, :] - jnp.take_along_axis(block_starts, chosen, axis=1)
    earlier = jnp.cumsum(counts, axis=0) - counts
    within = jnp.take_along_axis(earlier, chosen, axis=1) + within_own
    layout = jax.vmap(lambda single: jax.random.permutation(single, SEQ_DEV))(jax.random.split(place_key, block_total)).astype(jnp.int32)
    spots = layout[chosen, within]
    return (chosen * SEQ_DEV + spots).reshape(VIS).astype(jnp.int32)


def shard_levels(stream_key, extent, cuts, low, high):
    def one(axis_at, parts):
        heights = jax.random.uniform(jax.random.fold_in(jax.random.fold_in(stream_key, 6), axis_at), (parts,), jnp.float32, low / len(cuts), high / len(cuts))
        return jnp.repeat(jnp.exp(heights), extent[axis_at] // parts).reshape((-1,) + (1,) * (len(extent) - axis_at - 1))

    level = one(*cuts[0])
    for cut in cuts[1:]:
        level = level * one(*cut)
    return level


def length_profile(number_of, total, limit, slope):
    loads = [(1 << 20) // math.isqrt(grade ** slope) + 1 for grade in range(2, number_of + 1)]
    rest, given = total - limit - (number_of - 1), [1] * (number_of - 1)
    while rest > 0:
        candidates = [i for i in range(number_of - 1) if given[i] < limit]
        mass, budget = sum([loads[i] for i in candidates]), rest
        for i in candidates:
            addition = min(limit - given[i], max(1, budget * loads[i] // mass), rest)
            given[i] = given[i] + addition
            rest = rest - addition
    return np.array([limit] + given)


def uneven_parts(own_key, count, total, most, skew):
    if count == 2:
        one = jax.random.randint(own_key, (), max(1, total - most), min(most, total - 1) + 1)
        return jnp.stack([one, total - one])
    sizes = jnp.asarray(length_profile(count, total, most, skew), jnp.int32)
    pairs = (count - 1) // 2
    donor, receiver = sizes[1:1 + 2 * pairs:2], sizes[2:2 + 2 * pairs:2]
    slack = jnp.minimum(donor - 1, most - receiver)
    shifted = jax.random.randint(jax.random.fold_in(own_key, 1), (pairs,), 0, 1 << 20) % (slack + 1)
    sizes = sizes.at[1:1 + 2 * pairs:2].set(donor - shifted).at[2:2 + 2 * pairs:2].set(receiver + shifted)
    return sizes[jax.random.permutation(jax.random.fold_in(own_key, 2), count)]


def scatter_about(own_key, extent, width, most, shards=(), kind=jnp.bfloat16):
    loudness = shard_levels(own_key, extent, shards, -0.22, 0.18) if shards else 1.0
    entries = jax.random.normal(own_key, extent, jnp.float32) * width * loudness
    return jnp.minimum(jnp.maximum(entries, -most), most).astype(kind)


def setup_inputs(seed: int = 0) -> dict:
    seeds = jax.random.split(jax.random.key(seed), 14)
    patches = scatter_about(seeds[0], (PATCHES, D_VIT), 0.5, 4.0, ((0, 4),))
    vit_gain = jnp.clip(1.0 + 0.1 * jax.random.normal(seeds[1], (D_VIT,), jnp.float32), 0.5, 1.5)
    vision_qkv = draw_vision_qkv(jax.random.fold_in(seeds[13], 71), 0)
    vision_out = scatter_about(seeds[3], (D_VIT, D_VIT), D_VIT ** -0.5, 0.15625, ((0, 8),))
    video_ids = jnp.searchsorted(jnp.cumsum(uneven_parts(seeds[4], 3, VIS, 5 * VIS // 8, 0)), jnp.arange(VIS), side="right").astype(jnp.int32)
    merge_gain = jnp.clip(1.0 + 0.1 * jax.random.normal(seeds[5], (D_VIT,), jnp.float32), 0.5, 1.5)
    merge_up = scatter_about(seeds[6], (D_MRG, MRG_HID), D_MRG ** -0.5, 0.078125, ((1, 8),))
    merge_down = draw_merge_down(jax.random.fold_in(seeds[13], 71), 0)
    vision_pos = draw_vision_pos(jax.random.fold_in(seeds[13], 71), 0)
    text_embed = scatter_about(seeds[9], (SEQ, D), 1.0, 6.0, ((0, 32),))
    llm_gain = jnp.clip(1.0 + 0.1 * jax.random.normal(seeds[10], (D,), jnp.float32), 0.5, 1.5)
    query_weight = draw_query_weight(jax.random.fold_in(seeds[13], 71), 0)
    keyvalue_weight = draw_keyvalue_weight(jax.random.fold_in(seeds[13], 71), 0)
    return dict(patches=patches, vit_gain=vit_gain, vision_qkv=vision_qkv, vision_out=vision_out, video_ids=video_ids, merge_gain=merge_gain, merge_up=merge_up, merge_down=merge_down, vision_pos=vision_pos, text_embed=text_embed, llm_gain=llm_gain, query_weight=query_weight, keyvalue_weight=keyvalue_weight)


epsilon = 1e-06
rope_base = 1000000.0

def rms_scale(matrix, scales):
    widened = matrix.astype(jnp.float32)
    factor = lax.rsqrt(lax.optimization_barrier(jnp.mean(widened * widened, axis=-1, keepdims=True)) + epsilon)
    return widened * factor * scales

def rotary(tensor, positions):
    head_width = tensor.shape[-1]
    half_width = head_width // 2
    inverse = rope_base ** (-2.0 * jnp.arange(half_width, dtype=jnp.float32) / head_width)
    angles = positions.astype(jnp.float32)[:, None] * inverse[None, :]
    cosine = jnp.cos(angles)[:, None, :]
    sine_part = jnp.sin(angles)[:, None, :]
    first_half = tensor[..., :half_width]
    second_half = tensor[..., half_width:]
    return jnp.concatenate([first_half * cosine - second_half * sine_part, second_half * cosine + first_half * sine_part], axis=-1)

def attend_all(queries, key_rows, value_rows, allowed, score_scale):
    scores = jnp.dot(queries, key_rows.T, preferred_element_type=jnp.float32) * score_scale
    scores = jnp.where(allowed, scores, -jnp.inf)
    highest = lax.optimization_barrier(jnp.max(scores, axis=1, keepdims=True))
    weights = jnp.exp(scores - highest)
    row_sum = lax.optimization_barrier(jnp.sum(weights, axis=1, keepdims=True))
    mixed = jnp.dot(weights.astype(jnp.bfloat16), value_rows, preferred_element_type=jnp.float32)
    return mixed / row_sum

def reference(patches, vit_gain, vision_qkv, vision_out, video_ids, merge_gain, merge_up, merge_down, vision_pos, text_embed, llm_gain, query_weight, keyvalue_weight):
    normed_patches = rms_scale(patches, vit_gain).astype(jnp.bfloat16)
    projected = jnp.dot(normed_patches, vision_qkv, preferred_element_type=jnp.float32).astype(jnp.bfloat16)
    projected = projected.reshape(PATCHES, VIT_HEADS, 3, VIT_HDIM)
    stacked = jnp.transpose(projected, (2, 1, 0, 3))
    patch_video = jnp.repeat(video_ids, 4)
    same_video = patch_video[:, None] == patch_video[None, :]
    vit_heads_out = lax.map(lambda triple: attend_all(triple[0], triple[1], triple[2], same_video, VIT_HDIM ** (-0.5)), (stacked[0], stacked[1], stacked[2]))
    vit_context = jnp.transpose(vit_heads_out, (1, 0, 2)).reshape(PATCHES, D_VIT).astype(jnp.bfloat16)
    vit_output = patches.astype(jnp.float32) + jnp.dot(vit_context, vision_out, preferred_element_type=jnp.float32)
    merged_input = rms_scale(vit_output, merge_gain).astype(jnp.bfloat16).reshape(VIS, 4 * D_VIT)
    merge_hidden = jax.nn.gelu(jnp.dot(merged_input, merge_up, preferred_element_type=jnp.float32), approximate=False).astype(jnp.bfloat16)
    vision = jnp.dot(merge_hidden, merge_down, preferred_element_type=jnp.float32).astype(jnp.bfloat16)
    embedded = text_embed.at[vision_pos].set(vision)
    normed_tokens = rms_scale(embedded, llm_gain).astype(jnp.bfloat16)
    positions = jnp.arange(SEQ, dtype=jnp.int32)
    query_full = jnp.dot(normed_tokens, query_weight, preferred_element_type=jnp.float32).reshape(SEQ, KV_HEADS * QPK, HDIM)
    llm_query = rotary(query_full, positions).astype(jnp.bfloat16)
    pair_full = jnp.dot(normed_tokens, keyvalue_weight, preferred_element_type=jnp.float32).reshape(SEQ, KV_HEADS, 2, HDIM)
    llm_keys = rotary(pair_full[:, :, 0], positions).astype(jnp.bfloat16)
    llm_values = pair_full[:, :, 1].astype(jnp.bfloat16)
    causal = positions[:, None] >= positions[None, :]
    key_heads = jnp.repeat(jnp.transpose(llm_keys, (1, 0, 2)), QPK, axis=0)
    value_heads = jnp.repeat(jnp.transpose(llm_values, (1, 0, 2)), QPK, axis=0)
    llm_heads_out = lax.map(lambda triple: attend_all(triple[0], triple[1], triple[2], causal, HDIM ** (-0.5)), (jnp.transpose(llm_query, (1, 0, 2)), key_heads, value_heads))
    return jnp.transpose(llm_heads_out, (1, 0, 2)).reshape(SEQ, KV_HEADS * QPK * HDIM).astype(jnp.bfloat16)
```

```python
import math

import jax
import jax.numpy as jnp
from jax import lax
from jax.experimental import pallas as pl
from jax.experimental.pallas import tpu as pltpu
from jax.sharding import PartitionSpec as P

VIT_HDIM = 80
HDIM = 128


epsilon = 1e-06
rope_base = 1000000.0
lowest = -1e30
vmem_limit = 56 * 1024 * 1024


def rms_scale(matrix, scales):
    widened = matrix.astype(jnp.float32)
    factor = lax.rsqrt(jnp.mean(widened * widened, axis=-1, keepdims=True) + epsilon)
    return widened * factor * scales


def rotary(tensor, positions):
    head_width = tensor.shape[-1]
    half_width = head_width // 2
    inverse = rope_base ** (-2.0 * jnp.arange(half_width, dtype=jnp.float32) / head_width)
    angles = positions.astype(jnp.float32)[:, None] * inverse[None, :]
    cosine = jnp.cos(angles)[:, None, :]
    sine_part = jnp.sin(angles)[:, None, :]
    first_half = tensor[..., :half_width]
    second_half = tensor[..., half_width:]
    return jnp.concatenate(
        [
            first_half * cosine - second_half * sine_part,
            second_half * cosine + first_half * sine_part,
        ],
        axis=-1,
    )


def vit_attention_kernel(own_ref, ids_ref, q_ref, k_ref, v_ref, out_ref):
    allowed = own_ref[...] == ids_ref[...]
    parts = []
    for head in range(q_ref.shape[1] // VIT_HDIM):
        columns = slice(head * VIT_HDIM, (head + 1) * VIT_HDIM)
        scores = lax.dot_general(
            q_ref[:, columns],
            k_ref[:, columns],
            (((1,), (1,)), ((), ())),
            preferred_element_type=jnp.float32,
        )
        scores = jnp.where(allowed, scores, lowest)
        highest = jnp.max(scores, axis=1, keepdims=True)
        weights = jnp.exp((scores - highest) * VIT_HDIM ** (-0.5))
        row_sum = jnp.sum(weights, axis=1, keepdims=True)
        mixed = jnp.dot(
            weights.astype(jnp.bfloat16), v_ref[:, columns], preferred_element_type=jnp.float32
        )
        parts.append(mixed / row_sum)
    out_ref[...] = jnp.concatenate(parts, axis=1).astype(out_ref.dtype)


def vit_attention(own_ids, all_ids, queries, key_rows, value_rows):
    rows, width = queries.shape
    keys = key_rows.shape[0]
    step = math.gcd(rows, 256)
    return pl.pallas_call(
        vit_attention_kernel,
        grid=(rows // step,),
        in_specs=[
            pl.BlockSpec((step, 1), lambda i: (i, 0)),
            pl.BlockSpec((1, keys), lambda i: (0, 0)),
            pl.BlockSpec((step, width), lambda i: (i, 0)),
            pl.BlockSpec((keys, width), lambda i: (0, 0)),
            pl.BlockSpec((keys, width), lambda i: (0, 0)),
        ],
        out_specs=pl.BlockSpec((step, width), lambda i: (i, 0)),
        out_shape=jax.ShapeDtypeStruct((rows, width), jnp.bfloat16),
        compiler_params=pltpu.CompilerParams(vmem_limit_bytes=vmem_limit),
    )(own_ids[:, None], all_ids[None, :], queries, key_rows, value_rows)


def causal_kernel(block_ref, q_ref, k_ref, v_ref, out_ref):
    rows = q_ref.shape[0]
    queries = q_ref[...]

    def fold(start, state_in, masked):
        running_max, running_sum, weighted = state_in
        scores = lax.dot_general(
            queries,
            k_ref[pl.ds(start, rows), :],
            (((1,), (1,)), ((), ())),
            preferred_element_type=jnp.float32,
        )
        if masked:
            row_id = lax.broadcasted_iota(jnp.int32, (rows, rows), 0)
            column_id = lax.broadcasted_iota(jnp.int32, (rows, rows), 1)
            scores = jnp.where(row_id >= column_id, scores, lowest)
        new_max = jnp.maximum(running_max, jnp.max(scores, axis=1, keepdims=True))
        weights = jnp.exp((scores - new_max) * HDIM ** (-0.5))
        shrink = jnp.exp((running_max - new_max) * HDIM ** (-0.5))
        running_sum = running_sum * shrink + jnp.sum(weights, axis=1, keepdims=True)
        update = jnp.dot(
            weights.astype(jnp.bfloat16),
            v_ref[pl.ds(start, rows), :],
            preferred_element_type=jnp.float32,
        )
        return (new_max, running_sum, weighted * shrink + update)

    state = (
        jnp.full((rows, 1), lowest, jnp.float32),
        jnp.zeros((rows, 1), jnp.float32),
        jnp.zeros((rows, HDIM), jnp.float32),
    )
    own = block_ref[0]
    state = fold(pl.multiple_of(own * rows, rows), state, True)
    _, running_sum, weighted = lax.fori_loop(
        0, own, lambda i, now: fold(pl.multiple_of(i * rows, rows), now, False), state
    )
    out_ref[...] = (weighted / running_sum).astype(out_ref.dtype)


def causal_attention(block_index, queries, key_rows, value_rows):
    rows, width = queries.shape
    keys = key_rows.shape[0]
    return pl.pallas_call(
        causal_kernel,
        grid=(width // HDIM,),
        in_specs=[
            pl.BlockSpec(memory_space=pltpu.SMEM),
            pl.BlockSpec((rows, HDIM), lambda h: (0, h)),
            pl.BlockSpec((keys, HDIM), lambda h: (0, 0)),
            pl.BlockSpec((keys, HDIM), lambda h: (0, 0)),
        ],
        out_specs=pl.BlockSpec((rows, HDIM), lambda h: (0, h)),
        out_shape=jax.ShapeDtypeStruct((rows, width), jnp.bfloat16),
        compiler_params=pltpu.CompilerParams(vmem_limit_bytes=vmem_limit),
    )(block_index[None], queries, key_rows, value_rows)


def project(tokens, positions, query_weight, keyvalue_weight):
    rows = tokens.shape[0]
    query_full = jnp.dot(tokens, query_weight, preferred_element_type=jnp.float32)
    query = rotary(query_full.reshape(rows, -1, HDIM), positions).reshape(rows, -1)
    pair_full = jnp.dot(tokens, keyvalue_weight, preferred_element_type=jnp.float32)
    key = rotary(pair_full[:, :HDIM].reshape(rows, 1, HDIM), positions).reshape(rows, HDIM)
    pair = jnp.concatenate([key, pair_full[:, HDIM:]], axis=1)
    return query.astype(jnp.bfloat16), pair.astype(jnp.bfloat16)


def place(token_pos, first, text_rows, vision_rows):
    spots = first + jnp.arange(text_rows.shape[0], dtype=jnp.int32)
    hit = spots[:, None] == token_pos[None, :]
    moved = jnp.dot(hit.astype(jnp.bfloat16), vision_rows, preferred_element_type=jnp.float32)
    taken = jnp.any(hit, axis=1, keepdims=True)
    return jnp.where(taken, moved.astype(jnp.bfloat16), text_rows)


def local(
    patches,
    vit_gain,
    vision_qkv,
    vision_out,
    video_ids,
    merge_gain,
    merge_up,
    merge_down,
    vision_pos,
    text_embed,
    llm_gain,
    query_weight,
    keyvalue_weight,
):
    frame_index = lax.axis_index("frame")
    seq_index = lax.axis_index("seq")
    frame_count = lax.axis_size("frame")
    seq_count = lax.axis_size("seq")
    patch_rows = patches.shape[0]
    local_heads = vision_qkv.shape[1] // (3 * VIT_HDIM)
    normed_patches = rms_scale(patches, vit_gain).astype(jnp.bfloat16)
    projected = jnp.dot(normed_patches, vision_qkv, preferred_element_type=jnp.float32).astype(
        jnp.bfloat16
    )
    width = local_heads * VIT_HDIM
    projected = projected.reshape(patch_rows, local_heads, 3, VIT_HDIM)
    vit_query = projected[:, :, 0].reshape(patch_rows, width)
    vit_key = projected[:, :, 1].reshape(patch_rows, width)
    vit_value = projected[:, :, 2].reshape(patch_rows, width)
    patch_video = jnp.repeat(video_ids, 4)
    own_video = lax.dynamic_slice_in_dim(patch_video, frame_index * patch_rows, patch_rows)
    out_full = lax.all_gather(vision_out, "seq", axis=0, tiled=True)
    key_all = lax.all_gather(vit_key, "frame", axis=0, tiled=True)
    value_all = lax.all_gather(vit_value, "frame", axis=0, tiled=True)
    vit_context = vit_attention(own_video, patch_video, vit_query, key_all, value_all)
    context_all = lax.all_gather(vit_context.T, "seq", axis=0, tiled=True)
    head_total = lax.dot_general(
        context_all, out_full, (((0,), (0,)), ((), ())), preferred_element_type=jnp.float32
    )
    vit_output = patches.astype(jnp.float32) + head_total
    merged_input = (
        rms_scale(vit_output, merge_gain).astype(jnp.bfloat16).reshape(patch_rows // 4, -1)
    )
    merge_hidden = jax.nn.gelu(
        jnp.dot(merged_input, merge_up, preferred_element_type=jnp.float32), approximate=False
    ).astype(jnp.bfloat16)

    text_embed, context_tie = lax.optimization_barrier((text_embed, context_all))
    seq_block = text_embed.shape[0] * frame_count
    text_block = lax.all_gather(text_embed, "frame", axis=0, tiled=True)
    text_tokens = rms_scale(text_block, llm_gain).astype(jnp.bfloat16)
    first = seq_index * seq_block
    positions = first + jnp.arange(seq_block, dtype=jnp.int32)
    text_query, text_pair = project(text_tokens, positions, query_weight, keyvalue_weight)
    text_pair_all = lax.all_gather(text_pair, "seq", axis=0, tiled=True)

    vision_rows = lax.psum_scatter(
        jnp.dot(merge_hidden, merge_down, preferred_element_type=jnp.float32).astype(jnp.bfloat16),
        "seq",
        scatter_dimension=0,
        tiled=True,
    )
    share = vision_rows.shape[0]
    token_pos = vision_pos.reshape(frame_count, seq_count, share).transpose(1, 0, 2)
    vision_normed = rms_scale(vision_rows, llm_gain).astype(jnp.bfloat16)
    vision_tokens = lax.all_gather(vision_normed, "frame", axis=0, tiled=True)
    here = lax.dynamic_index_in_dim(token_pos, seq_index, 0, keepdims=False).reshape(-1)
    vision_query, vision_pair = project(vision_tokens, here, query_weight, keyvalue_weight)
    vision_all = lax.all_gather(
        jnp.concatenate([vision_query, vision_pair], axis=1), "seq", axis=0, tiled=True
    )
    token_pos = token_pos.reshape(-1)
    query_width = vision_query.shape[1]
    llm_query = place(token_pos, first, text_query, vision_all[:, :query_width])
    llm_pair = place(token_pos, 0, text_pair_all, vision_all[:, query_width:])
    return causal_attention(seq_index, llm_query, llm_pair[:, :HDIM], llm_pair[:, HDIM:])


def solution(mesh):
    return jax.shard_map(
        local,
        mesh=mesh,
        in_specs=(
            P("frame", None),
            P(),
            P(None, "seq"),
            P("seq", None),
            P(),
            P(),
            P(None, "seq"),
            P("seq", None),
            P(),
            P(("seq", "frame"), None),
            P(),
            P(None, "frame"),
            P(None, "frame"),
        ),
        out_specs=P("seq", "frame"),
        check_vma=False,
    )
```
